8 devices in a mesh: dp: 2 (over z, y), sp: 4 (over x, core).
Axes of the slice: x: 2, y: 2, z: 1, core: 2. Of those that a mesh axis runs over, the one named last changes fastest.
Arguments:
- latents: bfloat16 [32, 8, 64, 1280], P('dp', 'sp'), parts along dimension 0
- time_emb: bfloat16 [32, 1280], P('dp'), parts along dimension 0
- context: bfloat16 [32, 77, 2048], P('dp'), parts along dimension 0
- res_norm: float32 [2, 2, 2, 1280], replicated
- res_conv_w: bfloat16 [2, 2, 3, 3, 1280, 1280], replicated
- res_conv_b: float32 [2, 2, 1280], replicated
- res_temb_w: bfloat16 [2, 1280, 1280], replicated
- res_temb_b: float32 [2, 1280], replicated
- tr_norm: float32 [2, 1280], replicated
- proj_w: bfloat16 [2, 1280, 1280], replicated
- proj_b: float32 [2, 1280], replicated
- ln_par: float32 [2, 3, 2, 1280], replicated
- self_qkv: bfloat16 [2, 3, 1280, 20, 64], replicated
- cross_q: bfloat16 [2, 1280, 20, 64], replicated
- cross_kv: bfloat16 [2, 2, 2048, 20, 64], replicated
- attn_out: bfloat16 [2, 2, 20, 64, 1280], replicated
- attn_b: float32 [2, 2, 1280], replicated
- ff_in_w: bfloat16 [2, 1280, 10240], replicated
- ff_in_b: float32 [2, 10240], replicated
- ff_out_w: bfloat16 [2, 5120, 1280], replicated
- ff_out_b: float32 [2, 1280], replicated
Outputs:
- output: bfloat16 [32, 8, 64, 1280], P('dp', 'sp'), parts along dimension 0
There are 2 independent parts. The reference program is written for one: setup_inputs(seed, part) draws one part's arguments, and reference() takes and returns one part's arrays. A program takes and returns all parts, laid end to end along the dimension named above; an argument that names none is the same for every part.
All inputs are finite; a program needn't handle non-finite values.
Results may differ from the reference program's by a relative error of at most 0.0196347.
Values are sent between devices in bfloat16 or wider.
A program may use at most 1.25 GiB of HBM per device.

```python
import math
import jax
import jax.numpy as jnp
from jax import lax

IMG_BATCH = 16
IMG_ROWS = 8
IMG_WIDTH = 64
CHANNELS = 1280
NUM_HEADS = 20
TIME_DIM = 1280
CTX_DIM = 2048
CTX_LEN = 77
NUM_GROUPS = 32
FF_DIM = 5120

NUM_TOKENS = IMG_ROWS * IMG_WIDTH
HEAD_DIM = CHANNELS // NUM_HEADS
ATTN_SCALE = 1.0 / math.sqrt(HEAD_DIM)


def scaled_normal(rng_key, arr_shape, fan_in):
    return jax.random.normal(rng_key, arr_shape, jnp.float32) / math.sqrt(fan_in)


def setup_inputs(seed: int = 0, part: int = 0) -> dict:
    part_keys = jax.random.split(jax.random.fold_in(jax.random.key(seed + 1), part), 6)
    wt_keys = jax.random.split(jax.random.key(seed), 18)
    row_pos = jnp.arange(IMG_ROWS, dtype=jnp.float32)[None, :, None, None] * (math.pi / IMG_ROWS)
    mean_phase = jnp.repeat(jax.random.uniform(part_keys[0], (IMG_BATCH, 1, 1, NUM_GROUPS), jnp.float32, 0.0, 2.0 * math.pi), CHANNELS // NUM_GROUPS, axis=-1)
    scale_phase = jax.random.uniform(part_keys[1], (IMG_BATCH, 1, 1, CHANNELS), jnp.float32, 0.0, 2.0 * math.pi)
    chan_shift = 0.3 * jax.random.normal(part_keys[2], (IMG_BATCH, 1, 1, CHANNELS), jnp.float32)
    noise_val = jax.random.normal(part_keys[3], (IMG_BATCH, IMG_ROWS, IMG_WIDTH, CHANNELS), jnp.float32)
    latents = noise_val * (1.0 + 0.5 * jnp.cos(row_pos + scale_phase)) + 0.8 * jnp.sin(row_pos + mean_phase) + chan_shift
    time_emb = jax.random.normal(part_keys[4], (IMG_BATCH, TIME_DIM), jnp.float32)
    context = jax.random.normal(part_keys[5], (IMG_BATCH, CTX_LEN, CTX_DIM), jnp.float32)
    sharp_self = 0.8 * math.sqrt(math.log(NUM_TOKENS))
    sharp_cross = 0.8 * math.sqrt(math.log(CTX_LEN))
    affine_base = jnp.array([1.0, 0.0], jnp.float32)[:, None]
    qkv_gain = jnp.array([sharp_self, 1.0, 2.0], jnp.float32)[:, None, None, None]
    kv_gain = jnp.array([1.0, 2.0], jnp.float32)[:, None, None, None]
    return {
        'latents': latents.astype(jnp.bfloat16),
        'time_emb': time_emb.astype(jnp.bfloat16),
        'context': context.astype(jnp.bfloat16),
        'res_norm': affine_base + 0.25 * jax.random.normal(wt_keys[0], (2, 2, 2, CHANNELS), jnp.float32),
        'res_conv_w': scaled_normal(wt_keys[1], (2, 2, 3, 3, CHANNELS, CHANNELS), 9 * CHANNELS).astype(jnp.bfloat16),
        'res_conv_b': 0.3 * jax.random.normal(wt_keys[2], (2, 2, CHANNELS), jnp.float32),
        'res_temb_w': scaled_normal(wt_keys[3], (2, TIME_DIM, CHANNELS), TIME_DIM).astype(jnp.bfloat16),
        'res_temb_b': 0.3 * jax.random.normal(wt_keys[4], (2, CHANNELS), jnp.float32),
        'tr_norm': affine_base + 0.25 * jax.random.normal(wt_keys[5], (2, CHANNELS), jnp.float32),
        'proj_w': scaled_normal(wt_keys[6], (2, CHANNELS, CHANNELS), CHANNELS).astype(jnp.bfloat16),
        'proj_b': 0.3 * jax.random.normal(wt_keys[7], (2, CHANNELS), jnp.float32),
        'ln_par': affine_base + 0.25 * jax.random.normal(wt_keys[8], (2, 3, 2, CHANNELS), jnp.float32),
        'self_qkv': (scaled_normal(wt_keys[9], (2, 3, CHANNELS, NUM_HEADS, HEAD_DIM), CHANNELS) * qkv_gain).astype(jnp.bfloat16),
        'cross_q': (scaled_normal(wt_keys[10], (2, CHANNELS, NUM_HEADS, HEAD_DIM), CHANNELS) * sharp_cross).astype(jnp.bfloat16),
        'cross_kv': (scaled_normal(wt_keys[11], (2, 2, CTX_DIM, NUM_HEADS, HEAD_DIM), CTX_DIM) * kv_gain).astype(jnp.bfloat16),
        'attn_out': scaled_normal(wt_keys[12], (2, 2, NUM_HEADS, HEAD_DIM, CHANNELS), CHANNELS).astype(jnp.bfloat16),
        'attn_b': 0.3 * jax.random.normal(wt_keys[13], (2, 2, CHANNELS), jnp.float32),
        'ff_in_w': scaled_normal(wt_keys[14], (2, CHANNELS, 2 * FF_DIM), CHANNELS).astype(jnp.bfloat16),
        'ff_in_b': 0.3 * jax.random.normal(wt_keys[15], (2, 2 * FF_DIM), jnp.float32),
        'ff_out_w': scaled_normal(wt_keys[16], (2, FF_DIM, CHANNELS), FF_DIM).astype(jnp.bfloat16),
        'ff_out_b': 0.3 * jax.random.normal(wt_keys[17], (2, CHANNELS), jnp.float32),
    }


def matmul_f32(form, left, right):
    return jnp.einsum(form, left.astype(jnp.float32), right.astype(jnp.float32))


def group_norm(values, norm_gain, norm_bias, eps_val):
    grouped = values.astype(jnp.float32).reshape(IMG_BATCH, IMG_ROWS, IMG_WIDTH, NUM_GROUPS, CHANNELS // NUM_GROUPS)
    grp_mean = grouped.mean(axis=(1, 2, 4), keepdims=True)
    grp_sq = (grouped * grouped).mean(axis=(1, 2, 4), keepdims=True)
    normed = (grouped - grp_mean) * lax.rsqrt(grp_sq - grp_mean * grp_mean + eps_val)
    return normed.reshape(IMG_BATCH, IMG_ROWS, IMG_WIDTH, CHANNELS) * norm_gain + norm_bias


def conv_same(act_in, kernel):
    return lax.conv_general_dilated(act_in.astype(jnp.float32), kernel.astype(jnp.float32), (1, 1), 'SAME', dimension_numbers=('NHWC', 'HWIO', 'NHWC'))


def resnet(latents, time_emb, res_index, res_norm, res_conv_w, res_conv_b, res_temb_w, res_temb_b):
    first_act = jax.nn.silu(group_norm(latents, res_norm[res_index, 0, 0], res_norm[res_index, 0, 1], 1e-5)).astype(jnp.bfloat16)
    time_proj = jnp.dot(jax.nn.silu(time_emb.astype(jnp.float32)).astype(jnp.bfloat16), res_temb_w[res_index], preferred_element_type=jnp.float32) + res_temb_b[res_index]
    hidden = (conv_same(first_act, res_conv_w[res_index, 0]) + res_conv_b[res_index, 0] + time_proj[:, None, None, :]).astype(jnp.bfloat16)
    second_act = jax.nn.silu(group_norm(hidden, res_norm[res_index, 1, 0], res_norm[res_index, 1, 1], 1e-5)).astype(jnp.bfloat16)
    update = conv_same(second_act, res_conv_w[res_index, 1]) + res_conv_b[res_index, 1]
    return (latents.astype(jnp.float32) + update).astype(jnp.bfloat16)


def layer_norm(values, norm_gain, norm_bias):
    centered = values.astype(jnp.float32)
    centered = centered - centered.mean(axis=-1, keepdims=True)
    variance = (centered * centered).mean(axis=-1, keepdims=True)
    return (centered * lax.rsqrt(variance + 1e-5) * norm_gain + norm_bias).astype(jnp.bfloat16)


def attend_block(q_blk, k_all, v_all):
    scores = matmul_f32('bqhd,bkhd->bhqk', q_blk, k_all) * ATTN_SCALE
    row_exp = jnp.exp(scores - scores.max(axis=-1, keepdims=True))
    row_sum = row_exp.sum(axis=-1)
    row_out = matmul_f32('bhqk,bkhd->bqhd', row_exp.astype(jnp.bfloat16), v_all)
    return (row_out / jnp.swapaxes(row_sum, 1, 2)[..., None]).astype(jnp.bfloat16)


def transformer(hidden, context, tr_norm, proj_w, proj_b, ln_par, self_qkv, cross_q, cross_kv, attn_out, attn_b, ff_in_w, ff_in_b, ff_out_w, ff_out_b):
    normed = group_norm(hidden, tr_norm[0], tr_norm[1], 1e-6).astype(jnp.bfloat16).reshape(IMG_BATCH, NUM_TOKENS, CHANNELS)
    hidden_tok = (matmul_f32('bnc,cd->bnd', normed, proj_w[0]) + proj_b[0]).astype(jnp.bfloat16)

    def block_fn(carried, layer_w):
        ln_w, qkv_w, cq_w, ckv_w, out_w, out_b, ffi_w, ffi_b, ffo_w, ffo_b = layer_w
        normed_one = layer_norm(carried, ln_w[0, 0], ln_w[0, 1])
        q_all = matmul_f32('bnc,chd->bnhd', normed_one, qkv_w[0]).astype(jnp.bfloat16)
        k_all = matmul_f32('bnc,chd->bnhd', normed_one, qkv_w[1]).astype(jnp.bfloat16)
        v_all = matmul_f32('bnc,chd->bnhd', normed_one, qkv_w[2]).astype(jnp.bfloat16)
        q_rows = jnp.swapaxes(q_all.reshape(IMG_BATCH, IMG_ROWS, IMG_WIDTH, NUM_HEADS, HEAD_DIM), 0, 1)
        attended = lax.map(lambda q_row: attend_block(q_row, k_all, v_all), q_rows)
        attended = jnp.swapaxes(attended, 0, 1).reshape(IMG_BATCH, NUM_TOKENS, NUM_HEADS, HEAD_DIM)
        carried = (carried.astype(jnp.float32) + matmul_f32('bnhd,hdc->bnc', attended, out_w[0]) + out_b[0]).astype(jnp.bfloat16)
        normed_two = layer_norm(carried, ln_w[1, 0], ln_w[1, 1])
        q_cross = matmul_f32('bnc,chd->bnhd', normed_two, cq_w).astype(jnp.bfloat16)
        k_cross = matmul_f32('btc,chd->bthd', context, ckv_w[0]).astype(jnp.bfloat16)
        v_cross = matmul_f32('btc,chd->bthd', context, ckv_w[1]).astype(jnp.bfloat16)
        crossed = attend_block(q_cross, k_cross, v_cross)
        carried = (carried.astype(jnp.float32) + matmul_f32('bnhd,hdc->bnc', crossed, out_w[1]) + out_b[1]).astype(jnp.bfloat16)
        normed_three = layer_norm(carried, ln_w[2, 0], ln_w[2, 1])
        ff_proj = matmul_f32('bnc,cf->bnf', normed_three, ffi_w) + ffi_b
        gated_act = (ff_proj[..., :FF_DIM] * jax.nn.gelu(ff_proj[..., FF_DIM:], approximate=False)).astype(jnp.bfloat16)
        carried = (carried.astype(jnp.float32) + matmul_f32('bnf,fc->bnc', gated_act, ffo_w) + ffo_b).astype(jnp.bfloat16)
        return carried, None

    hidden_tok, _unused = lax.scan(block_fn, hidden_tok, (ln_par, self_qkv, cross_q, cross_kv, attn_out, attn_b, ff_in_w, ff_in_b, ff_out_w, ff_out_b))
    out_tok = matmul_f32('bnc,cd->bnd', hidden_tok, proj_w[1]) + proj_b[1] + hidden.reshape(IMG_BATCH, NUM_TOKENS, CHANNELS).astype(jnp.float32)
    return out_tok.astype(jnp.bfloat16).reshape(IMG_BATCH, IMG_ROWS, IMG_WIDTH, CHANNELS)


def reference(latents, time_emb, context, res_norm, res_conv_w, res_conv_b, res_temb_w, res_temb_b, tr_norm, proj_w, proj_b, ln_par, self_qkv, cross_q, cross_kv, attn_out, attn_b, ff_in_w, ff_in_b, ff_out_w, ff_out_b):
    first_out = resnet(latents, time_emb, 0, res_norm, res_conv_w, res_conv_b, res_temb_w, res_temb_b)
    middle = transformer(first_out, context, tr_norm, proj_w, proj_b, ln_par, self_qkv, cross_q, cross_kv, attn_out, attn_b, ff_in_w, ff_in_b, ff_out_w, ff_out_b)
    return resnet(middle, time_emb, 1, res_norm, res_conv_w, res_conv_b, res_temb_w, res_temb_b)
```

```python
import functools
import math
import jax
import jax.numpy as jnp
from jax import lax
from jax.sharding import PartitionSpec as P

NUM_GROUPS = 32


def group_norm(values, norm_gain, norm_bias, eps_val):
    batch_n, rows_n, cols_n, chan_n = values.shape
    grouped = values.astype(jnp.float32).reshape(batch_n, rows_n, cols_n, NUM_GROUPS, chan_n // NUM_GROUPS)
    count_n = rows_n * cols_n * (chan_n // NUM_GROUPS)
    grp_mean = grouped.sum(axis=(1, 2, 4)) / count_n
    grp_var = (grouped * grouped).sum(axis=(1, 2, 4)) / count_n - grp_mean * grp_mean
    inv_std = lax.rsqrt(grp_var + eps_val)
    normed = (grouped - grp_mean[:, None, None, :, None]) * inv_std[:, None, None, :, None]
    return normed.reshape(batch_n, rows_n, cols_n, chan_n) * norm_gain + norm_bias


def conv_rows(act_in, kernel):
    return lax.conv_general_dilated(act_in, kernel, (1, 1), ((1, 1), (1, 1)), dimension_numbers=('NHWC', 'HWIO', 'NHWC'), preferred_element_type=jnp.float32)


def resnet_local(latents, time_emb, res_index, res_norm, res_conv_w, res_conv_b, res_temb_w, res_temb_b):
    first_act = jax.nn.silu(group_norm(latents, res_norm[res_index, 0, 0], res_norm[res_index, 0, 1], 1e-5)).astype(jnp.bfloat16)
    time_proj = jnp.dot(jax.nn.silu(time_emb.astype(jnp.float32)).astype(jnp.bfloat16), res_temb_w[res_index], preferred_element_type=jnp.float32) + res_temb_b[res_index]
    hidden = (conv_rows(first_act, res_conv_w[res_index, 0]) + res_conv_b[res_index, 0] + time_proj[:, None, None, :]).astype(jnp.bfloat16)
    second_act = jax.nn.silu(group_norm(hidden, res_norm[res_index, 1, 0], res_norm[res_index, 1, 1], 1e-5)).astype(jnp.bfloat16)
    update = conv_rows(second_act, res_conv_w[res_index, 1]) + res_conv_b[res_index, 1]
    return (latents.astype(jnp.float32) + update).astype(jnp.bfloat16)


def layer_norm(values, norm_gain, norm_bias):
    centered = values.astype(jnp.float32)
    centered = centered - centered.mean(axis=-1, keepdims=True)
    variance = (centered * centered).mean(axis=-1, keepdims=True)
    return (centered * lax.rsqrt(variance + 1e-5) * norm_gain + norm_bias).astype(jnp.bfloat16)


def attend_block(q_blk, k_all, v_all):
    scale_f = 1.0 / math.sqrt(q_blk.shape[-1])
    scores = jnp.einsum('bqhd,bkhd->bhqk', q_blk, k_all, preferred_element_type=jnp.float32) * scale_f
    row_exp = jnp.exp(scores - scores.max(axis=-1, keepdims=True))
    row_sum = row_exp.sum(axis=-1)
    row_out = jnp.einsum('bhqk,bkhd->bqhd', row_exp.astype(jnp.bfloat16), v_all, preferred_element_type=jnp.float32)
    return (row_out / jnp.swapaxes(row_sum, 1, 2)[..., None]).astype(jnp.bfloat16)


def transformer_local(hidden, context, tr_norm, proj_w, proj_b, ln_par, self_qkv, cross_q, cross_kv, attn_out, attn_b, ff_in_w, ff_in_b, ff_out_w, ff_out_b):
    batch_n, rows_n, cols_n, chan_n = hidden.shape
    normed = group_norm(hidden, tr_norm[0], tr_norm[1], 1e-6).astype(jnp.bfloat16).reshape(batch_n, rows_n * cols_n, chan_n)
    hidden_tok = (jnp.einsum('bnc,cd->bnd', normed, proj_w[0], preferred_element_type=jnp.float32) + proj_b[0]).astype(jnp.bfloat16)
    ff_width = ff_out_w.shape[1]
    for layer_i in range(ln_par.shape[0]):
        normed = layer_norm(hidden_tok, ln_par[layer_i, 0, 0], ln_par[layer_i, 0, 1])
        qkv_loc = jnp.einsum('bnc,jchd->jbnhd', normed, self_qkv[layer_i], preferred_element_type=jnp.float32).astype(jnp.bfloat16)
        attended = attend_block(qkv_loc[0], qkv_loc[1], qkv_loc[2])
        hidden_tok = (hidden_tok.astype(jnp.float32) + jnp.einsum('bnhd,hdc->bnc', attended, attn_out[layer_i, 0], preferred_element_type=jnp.float32) + attn_b[layer_i, 0]).astype(jnp.bfloat16)
        normed = layer_norm(hidden_tok, ln_par[layer_i, 1, 0], ln_par[layer_i, 1, 1])
        q_cross = jnp.einsum('bnc,chd->bnhd', normed, cross_q[layer_i], preferred_element_type=jnp.float32).astype(jnp.bfloat16)
        kv_cross = jnp.einsum('btc,jchd->jbthd', context, cross_kv[layer_i], preferred_element_type=jnp.float32).astype(jnp.bfloat16)
        crossed = attend_block(q_cross, kv_cross[0], kv_cross[1])
        hidden_tok = (hidden_tok.astype(jnp.float32) + jnp.einsum('bnhd,hdc->bnc', crossed, attn_out[layer_i, 1], preferred_element_type=jnp.float32) + attn_b[layer_i, 1]).astype(jnp.bfloat16)
        normed = layer_norm(hidden_tok, ln_par[layer_i, 2, 0], ln_par[layer_i, 2, 1])
        ff_proj = jnp.einsum('bnc,cf->bnf', normed, ff_in_w[layer_i], preferred_element_type=jnp.float32) + ff_in_b[layer_i]
        gated_act = (ff_proj[..., :ff_width] * jax.nn.gelu(ff_proj[..., ff_width:], approximate=False)).astype(jnp.bfloat16)
        hidden_tok = (hidden_tok.astype(jnp.float32) + jnp.einsum('bnf,fc->bnc', gated_act, ff_out_w[layer_i], preferred_element_type=jnp.float32) + ff_out_b[layer_i]).astype(jnp.bfloat16)
    out_tok = jnp.einsum('bnc,cd->bnd', hidden_tok, proj_w[1], preferred_element_type=jnp.float32) + proj_b[1] + hidden.reshape(batch_n, rows_n * cols_n, chan_n).astype(jnp.float32)
    return out_tok.astype(jnp.bfloat16).reshape(batch_n, rows_n, cols_n, chan_n)


def device_block(latents, time_emb, context, res_norm, res_conv_w, res_conv_b, res_temb_w, res_temb_b, tr_norm, proj_w, proj_b, ln_par, self_qkv, cross_q, cross_kv, attn_out, attn_b, ff_in_w, ff_in_b, ff_out_w, ff_out_b, sp_size):
    own_n = latents.shape[0] // sp_size
    first = lax.axis_index('sp') * own_n
    whole = lax.all_to_all(latents, 'sp', 0, 1, tiled=True)
    time_own = lax.dynamic_slice_in_dim(time_emb, first, own_n, 0)
    ctx_own = lax.dynamic_slice_in_dim(context, first, own_n, 0)
    first_out = resnet_local(whole, time_own, 0, res_norm, res_conv_w, res_conv_b, res_temb_w, res_temb_b)
    middle = transformer_local(first_out, ctx_own, tr_norm, proj_w, proj_b, ln_par, self_qkv, cross_q, cross_kv, attn_out, attn_b, ff_in_w, ff_in_b, ff_out_w, ff_out_b)
    last = resnet_local(middle, time_own, 1, res_norm, res_conv_w, res_conv_b, res_temb_w, res_temb_b)
    return lax.all_to_all(last, 'sp', 1, 0, tiled=True)


def solution(mesh):
    sp_size = mesh.shape['sp']
    row_spec = P('dp', 'sp')
    part_spec = P('dp')
    in_specs = (row_spec, part_spec, part_spec) + (P(),) * 18
    body_fn = functools.partial(device_block, sp_size=sp_size)
    return jax.shard_map(body_fn, mesh=mesh, in_specs=in_specs, out_specs=row_spec, check_vma=False)
```

```python
import functools
import math
import jax
import jax.numpy as jnp
import numpy as np
from jax import lax
from jax.experimental import pallas as pl
from jax.experimental.pallas import tpu as pltpu
from jax.sharding import PartitionSpec as P

BF = jnp.bfloat16
F32 = jnp.float32
NUM_GROUPS = 32
WIDTH = 64
CBLK = 256
VMEM_CAP = 63 << 20


def mm(lhs, rhs):
    return jnp.dot(lhs, rhs, preferred_element_type=F32)


def split_rows(first, second):
    parts = []
    for row in (first, second):
        high = row.astype(BF).astype(F32)
        rest = row - high
        mid = rest.astype(BF).astype(F32)
        parts += [high, mid, rest - mid]
    parts += [jnp.zeros_like(first)] * 2
    return jnp.concatenate(parts, 0).astype(BF)


def group_tables(chan_n):
    member = np.zeros((chan_n, 128), np.float32)
    member[np.arange(chan_n), np.arange(chan_n) // (chan_n // NUM_GROUPS)] = 1.0
    return jnp.asarray(member, BF), jnp.asarray(member.T, BF)


def group_scale(chan_sum, chan_sq, to_group, to_chan, count_n, eps_val):
    sums = mm(split_rows(chan_sum, chan_sq), to_group)
    mean = (sums[0:1] + sums[1:2] + sums[2:3]) / count_n
    square = (sums[3:4] + sums[4:5] + sums[5:6]) / count_n
    inv_std = lax.rsqrt(square - mean * mean + eps_val)
    wide = mm(split_rows(mean, inv_std), to_chan)
    return wide[0:1] + wide[1:2] + wide[2:3], wide[3:4] + wide[4:5] + wide[5:6]


def latent_stats(src_ref):
    rows_n, chan_n = src_ref.shape
    sums, squares = [], []
    for col in range(0, chan_n, CBLK):
        part_sum, part_sq = 0.0, 0.0
        for row in range(0, rows_n, WIDTH):
            blk = src_ref[row:row + WIDTH, col:col + CBLK].astype(F32)
            blk = blk.reshape(WIDTH // 8, 8, CBLK)
            part_sum = part_sum + blk.sum(0)
            part_sq = part_sq + (blk * blk).sum(0)
        sums.append(part_sum.sum(0, keepdims=True))
        squares.append(part_sq.sum(0, keepdims=True))
    return jnp.concatenate(sums, 1), jnp.concatenate(squares, 1)


def silu(val):
    half = 0.5 * val
    return half + half * jnp.tanh(half)


def norm_latent(src_ref, dst_ref, gain, bias, to_group, to_chan, eps_val, spread):
    rows_n, chan_n = src_ref.shape
    chan_sum, chan_sq = latent_stats(src_ref)
    mean, inv_std = group_scale(chan_sum, chan_sq, to_group, to_chan, rows_n * (chan_n // NUM_GROUPS), eps_val)
    scale = inv_std * gain
    col_pos = lax.broadcasted_iota(jnp.int32, (WIDTH, CBLK), 0)
    for row in range(0, rows_n, WIDTH):
        for col in range(0, chan_n, CBLK):
            cols = slice(col, col + CBLK)
            val = (src_ref[row:row + WIDTH, cols].astype(F32) - mean[:, cols]) * scale[:, cols] + bias[:, cols]
            rows = slice(row, row + WIDTH)
            if not spread:
                dst_ref[rows, cols] = val.astype(BF)
                continue
            act = silu(val)
            before = jnp.where(col_pos == 0, 0.0, pltpu.roll(act, 1, 0))
            after = jnp.where(col_pos == WIDTH - 1, 0.0, pltpu.roll(act, WIDTH - 1, 0))
            dst_ref[rows, cols] = before.astype(BF)
            dst_ref[rows, chan_n + col:chan_n + col + CBLK] = act.astype(BF)
            dst_ref[rows, 2 * chan_n + col:2 * chan_n + col + CBLK] = after.astype(BF)


def affine(norm_ref, at):
    return norm_ref[at + (slice(0, 1),)], norm_ref[at + (slice(1, 2),)]


def prep_kernel(x_ref, norm_ref, tog_ref, toc_ref, o_ref, *, eps_val, at):
    norm_latent(x_ref, o_ref, *affine(norm_ref, at), tog_ref[...], toc_ref[...], eps_val, True)


HBM_SPEC = pl.BlockSpec(memory_space=pl.ANY)


def params():
    return pltpu.CompilerParams(vmem_limit_bytes=VMEM_CAP)


def whole(shape):
    return pl.BlockSpec(shape, lambda *_: (0,) * len(shape), pipeline_mode=pl.Buffered(1))


def prep_call(x, norm, at, eps_val):
    lat_n, rows_n, chan_n = x.shape
    to_group, to_chan = group_tables(chan_n)
    return pl.pallas_call(
        functools.partial(prep_kernel, eps_val=eps_val, at=at),
        grid=(lat_n,),
        in_specs=[pl.BlockSpec((None, rows_n, chan_n), lambda i: (i, 0, 0)), whole(norm.shape), whole((chan_n, 128)), whole((128, chan_n))],
        out_specs=pl.BlockSpec((None, rows_n, 3 * chan_n), lambda i: (i, 0, 0)),
        out_shape=jax.ShapeDtypeStruct((lat_n, rows_n, 3 * chan_n), BF),
        compiler_params=params(),
        name='prep',
    )(x, norm, to_group, to_chan)


def conv_kernel(*refs, lat_n, slot, eps_val, timed, residual, spread, normed, at):
    refs = list(refs)
    x3_ref, w_hbm, cb_ref = refs[:3]
    refs = refs[3:]
    time_ref = refs.pop(0) if timed else None
    res_ref = refs.pop(0) if residual else None
    if normed:
        norm_ref, tog_ref, toc_ref = refs[:3]
        refs = refs[3:]
    out_ref = refs.pop(0) if residual else None
    nrm_ref = refs.pop(0) if normed else None
    w_buf, sems, held = refs
    rows_n, chan_n = held.shape
    step = pl.program_id(0)
    third = 3 * chan_n

    parts = [(third + i * chan_n, chan_n) for i in range(3)] + [(0, third), (2 * third, third)]

    def fetch(i):
        first, size = parts[i]
        return pltpu.make_async_copy(w_hbm.at[slot, pl.ds(first, size)], w_buf.at[pl.ds(first, size)], sems.at[i])

    def convolve(first_time):
        def ready(i):
            if first_time:
                fetch(i).wait()
        if first_time:
            ready(0)
            mid = mm(x3_ref[:, 0:chan_n], w_buf[third:third + chan_n])
            ready(1)
            mid = mid + mm(x3_ref[:, chan_n:2 * chan_n], w_buf[third + chan_n:third + 2 * chan_n])
            ready(2)
            mid = mid + mm(x3_ref[:, 2 * chan_n:], w_buf[third + 2 * chan_n:2 * third])
        else:
            mid = mm(x3_ref[...], w_buf[third:2 * third])
        ready(3)
        upper = mm(x3_ref[0:rows_n - WIDTH, :], w_buf[0:third])
        ready(4)
        lower = mm(x3_ref[WIDTH:rows_n, :], w_buf[2 * third:3 * third])
        last = rows_n - WIDTH
        for rows, val in (
            (slice(0, WIDTH), mid[0:WIDTH] + lower[0:WIDTH]),
            (slice(WIDTH, last), mid[WIDTH:last] + upper[0:last - WIDTH] + lower[WIDTH:last]),
            (slice(last, rows_n), mid[last:] + upper[last - WIDTH:]),
        ):
            val = val + cb_ref[slot // 2, slot % 2:slot % 2 + 1, :]
            if timed:
                val = val + time_ref[...]
            if residual:
                val = res_ref[rows, :].astype(F32) + val
            val = val.astype(BF)
            if normed:
                held[rows, :] = val
            if residual:
                out_ref[rows, :] = val

    def finish():
        norm_latent(held, nrm_ref, *affine(norm_ref, at), tog_ref[...], toc_ref[...], eps_val, spread)

    @pl.when(step == 0)
    def _():
        for i in range(len(parts)):
            fetch(i).start()
        convolve(True)

    @pl.when((step > 0) & (step < lat_n))
    def _():
        if normed:
            finish()
        convolve(False)

    if normed:
        @pl.when(step == lat_n)
        def _():
            finish()


def conv_call(x3, w_all, slot, conv_b, time_row, res, norm, at, eps_val, spread):
    lat_n, rows_n, wide = x3.shape
    chan_n = wide // 3
    timed, residual, normed = time_row is not None, res is not None, norm is not None
    here = lambda i: (jnp.minimum(i, lat_n - 1), 0, 0)
    prev = lambda i: (jnp.maximum(i - 1, 0), 0, 0)
    args = [x3, w_all, conv_b]
    in_specs = [pl.BlockSpec((None, rows_n, wide), here), HBM_SPEC, whole(conv_b.shape)]
    out_specs, out_shape = [], []
    if timed:
        args.append(time_row)
        in_specs.append(pl.BlockSpec((None, 1, chan_n), here))
    if residual:
        args.append(res)
        in_specs.append(pl.BlockSpec((None, rows_n, chan_n), here))
        out_specs.append(pl.BlockSpec((None, rows_n, chan_n), here))
        out_shape.append(jax.ShapeDtypeStruct((lat_n, rows_n, chan_n), BF))
    if normed:
        to_group, to_chan = group_tables(chan_n)
        args += [norm, to_group, to_chan]
        in_specs += [whole(norm.shape), whole((chan_n, 128)), whole((128, chan_n))]
        out_n = wide if spread else chan_n
        out_specs.append(pl.BlockSpec((None, rows_n, out_n), prev))
        out_shape.append(jax.ShapeDtypeStruct((lat_n, rows_n, out_n), BF))
    flops = 2 * lat_n * rows_n * chan_n * wide * 3
    outs = pl.pallas_call(
        functools.partial(conv_kernel, lat_n=lat_n, slot=slot, eps_val=eps_val, timed=timed, residual=residual, spread=spread, normed=normed, at=at),
        grid=(lat_n + (1 if normed else 0),),
        in_specs=in_specs, out_specs=out_specs, out_shape=out_shape,
        scratch_shapes=[pltpu.VMEM((3 * wide, chan_n), BF), pltpu.SemaphoreType.DMA((5,)), pltpu.VMEM((rows_n, chan_n), BF)],
        compiler_params=params(),
        cost_estimate=pl.CostEstimate(flops=flops, bytes_accessed=3 * wide * chan_n * 2, transcendentals=0),
        name='conv',
    )(*args)
    return outs


LN_ROWS = 32
LOG2E = math.log2(math.e)


def mm_t(lhs, rhs):
    return lax.dot_general(lhs, rhs, (((1,), (1,)), ((), ())), preferred_element_type=F32)


def norm_rows(src_ref, dst_ref, gain, bias):
    for row in range(0, src_ref.shape[0], LN_ROWS):
        rows = slice(row, row + LN_ROWS)
        val = src_ref[rows, :].astype(F32)
        val = val - val.mean(-1, keepdims=True)
        var = (val * val).mean(-1, keepdims=True)
        dst_ref[rows, :] = (val * lax.rsqrt(var + 1e-5) * gain + bias).astype(BF)


def lat_spec(shape, lat_n, lag):
    return pl.BlockSpec((None,) + shape, lambda i: (jnp.clip(i - lag, 0, lat_n - 1),) + (0,) * len(shape))


def enter_kernel(n_ref, pw_hbm, pb_ref, ln_ref, qw_hbm, u_ref, qkv_ref, pw_buf, qw_buf, held, nrm, sems, *, lat_n, layer):
    step = pl.program_id(0)
    chan_n = held.shape[1]
    half = chan_n // 2
    copies = [pltpu.make_async_copy(pw_hbm.at[0, pl.ds(i * half, half)], pw_buf.at[pl.ds(i * half, half)], sems.at[i]) for i in range(2)]
    copies += [pltpu.make_async_copy(qw_hbm.at[layer, j], qw_buf.at[j], sems.at[2 + j]) for j in range(3)]

    def project(first):
        if first:
            copies[0].wait()
            val = mm(n_ref[:, 0:half], pw_buf[0:half])
            copies[1].wait()
            val = val + mm(n_ref[:, half:], pw_buf[half:])
        else:
            val = mm(n_ref[...], pw_buf[...])
        val = (val + pb_ref[0:1, :]).astype(BF)
        held[...] = val
        u_ref[...] = val

    def norm():
        norm_rows(held, nrm, *affine(ln_ref, (layer, 0)))

    def heads(first=False):
        for j in range(3):
            if first:
                copies[2 + j].wait()
            qkv_ref[:, j * chan_n:(j + 1) * chan_n] = mm_t(nrm[...], qw_buf[j]).astype(BF)

    @pl.when(step == 0)
    def _():
        for cp in copies:
            cp.start()
        project(True)

    @pl.when(step == 1)
    def _():
        norm()
        project(False)

    @pl.when(step == 2)
    def _():
        heads(True)
        norm()
        project(False)

    @pl.when((step > 2) & (step < lat_n))
    def _():
        heads()
        norm()
        project(False)

    @pl.when(step == lat_n)
    def _():
        heads()
        norm()

    @pl.when(step == lat_n + 1)
    def _():
        heads()


def enter_call(nrm_in, proj_w, proj_b, ln_par, qkv_t, layer):
    lat_n, rows_n, chan_n = nrm_in.shape
    return pl.pallas_call(
        functools.partial(enter_kernel, lat_n=lat_n, layer=layer),
        grid=(lat_n + 2,),
        in_specs=[lat_spec((rows_n, chan_n), lat_n, 0), HBM_SPEC, whole(proj_b.shape), whole(ln_par.shape), HBM_SPEC],
        out_specs=[lat_spec((rows_n, chan_n), lat_n, 0), lat_spec((rows_n, 3 * chan_n), lat_n, 2)],
        out_shape=[jax.ShapeDtypeStruct((lat_n, rows_n, chan_n), BF), jax.ShapeDtypeStruct((lat_n, rows_n, 3 * chan_n), BF)],
        scratch_shapes=[pltpu.VMEM((chan_n, chan_n), BF), pltpu.VMEM((3, chan_n, chan_n), BF), pltpu.VMEM((rows_n, chan_n), BF), pltpu.VMEM((rows_n, chan_n), BF), pltpu.SemaphoreType.DMA((5,))],
        compiler_params=params(),
        cost_estimate=pl.CostEstimate(flops=8 * lat_n * rows_n * chan_n * chan_n, bytes_accessed=8 * chan_n * chan_n, transcendentals=0),
        name='enter',
    )(nrm_in, proj_w, proj_b, ln_par, qkv_t)


def heads_kernel(u_ref, ln_ref, qw_hbm, qkv_ref, qw_buf, nrm, sems, *, lat_n, layer):
    step = pl.program_id(0)
    chan_n = nrm.shape[1]
    copies = [pltpu.make_async_copy(qw_hbm.at[layer, j], qw_buf.at[j], sems.at[j]) for j in range(3)]

    def norm():
        norm_rows(u_ref, nrm, *affine(ln_ref, (layer, 0)))

    def heads(first=False):
        for j in range(3):
            if first:
                copies[j].wait()
            qkv_ref[:, j * chan_n:(j + 1) * chan_n] = mm_t(nrm[...], qw_buf[j]).astype(BF)

    @pl.when(step == 0)
    def _():
        for cp in copies:
            cp.start()
        norm()

    @pl.when(step == 1)
    def _():
        heads(True)
        norm()

    @pl.when((step > 1) & (step < lat_n))
    def _():
        heads()
        norm()

    @pl.when(step == lat_n)
    def _():
        heads()


def heads_call(u, ln_par, qkv_t, layer):
    lat_n, rows_n, chan_n = u.shape
    return pl.pallas_call(
        functools.partial(heads_kernel, lat_n=lat_n, layer=layer),
        grid=(lat_n + 1,),
        in_specs=[lat_spec((rows_n, chan_n), lat_n, 0), whole(ln_par.shape), HBM_SPEC],
        out_specs=lat_spec((rows_n, 3 * chan_n), lat_n, 1),
        out_shape=jax.ShapeDtypeStruct((lat_n, rows_n, 3 * chan_n), BF),
        scratch_shapes=[pltpu.VMEM((3, chan_n, chan_n), BF), pltpu.VMEM((rows_n, chan_n), BF), pltpu.SemaphoreType.DMA((3,))],
        compiler_params=params(),
        cost_estimate=pl.CostEstimate(flops=6 * lat_n * rows_n * chan_n * chan_n, bytes_accessed=6 * chan_n * chan_n, transcendentals=0),
        name='heads',
    )(u, ln_par, qkv_t)


HEAD_DIM = 64
PAIR = 2 * HEAD_DIM
EXP_SCALE = LOG2E / math.sqrt(HEAD_DIM)


def attn_kernel(q_ref, k_ref, v_ref, o_ref, *, q_rows):
    rows_n, chan_n = q_ref.shape
    left = lax.broadcasted_iota(jnp.int32, (q_rows, PAIR), 1) < HEAD_DIM

    def scores(unit):
        cols, rows = unit
        q = q_ref[rows, cols]
        zero = jnp.zeros_like(q)
        return mm_t(jnp.where(left, q, zero), k_ref[:, cols]), mm_t(jnp.where(left, zero, q), k_ref[:, cols])

    def finish(unit, pair):
        cols, rows = unit
        outs = []
        for s in pair:
            e = jnp.exp2((s - s.max(-1, keepdims=True)) * EXP_SCALE)
            outs.append(mm(e.astype(BF), v_ref[:, cols]) / e.sum(-1, keepdims=True))
        o_ref[rows, cols] = jnp.where(left, outs[0], outs[1]).astype(BF)

    units = [(slice(c, c + PAIR), slice(r, r + q_rows)) for c in range(0, chan_n, PAIR) for r in range(0, rows_n, q_rows)]
    waiting = None
    for unit in units:
        pair = scores(unit)
        if waiting is not None:
            finish(*waiting)
        waiting = (unit, pair)
    finish(*waiting)


def attn_call(qkv):
    lat_n, rows_n, wide = qkv.shape
    chan_n = wide // 3
    return pl.pallas_call(
        functools.partial(attn_kernel, q_rows=256),
        grid=(lat_n,),
        in_specs=[pl.BlockSpec((None, rows_n, chan_n), lambda i, j=j: (i, 0, j)) for j in range(3)],
        out_specs=pl.BlockSpec((None, rows_n, chan_n), lambda i: (i, 0, 0)),
        out_shape=jax.ShapeDtypeStruct((lat_n, rows_n, chan_n), BF),
        compiler_params=params(),
        cost_estimate=pl.CostEstimate(flops=16 * lat_n * rows_n * rows_n * chan_n, bytes_accessed=8 * lat_n * rows_n * chan_n, transcendentals=0),
        name='attn',
    )(qkv, qkv, qkv)


KEY_PAD = 128


def mix_kernel(o_ref, u_ref, kc_ref, vc_ref, ow_hbm, ob_ref, qw_hbm, ln_ref, u_out, n_out, ow_buf, cw_buf, qw_buf, mid, mid_old, nrm, crossed, sems, *, lat_n, layer, key_n):
    step = pl.program_id(0)
    rows_n, chan_n = mid.shape
    copies = [pltpu.make_async_copy(ow_hbm.at[layer, 0], ow_buf, sems.at[0]), pltpu.make_async_copy(qw_hbm.at[layer], qw_buf, sems.at[1]), pltpu.make_async_copy(ow_hbm.at[layer, 1], cw_buf, sems.at[2])]

    def leave(first=False):
        if first:
            copies[2].wait()
        val = mid_old[...].astype(F32) + (mm(crossed[...], cw_buf[...]) + ob_ref[layer, 1:2, :])
        u_out[...] = val.astype(BF)
        norm_rows(u_out, n_out, *affine(ln_ref, (layer, 2)))

    def cross(first=False):
        if first:
            copies[1].wait()
        q_all = mm_t(nrm[...], qw_buf[...]).astype(BF)
        key_rows = kc_ref.shape[0]
        key_left = lax.broadcasted_iota(jnp.int32, (key_rows, PAIR), 1) < HEAD_DIM
        valid = lax.broadcasted_iota(jnp.int32, (rows_n, KEY_PAD), 1) < key_n
        left = lax.broadcasted_iota(jnp.int32, (rows_n, PAIR), 1) < HEAD_DIM
        zero = jnp.zeros((key_rows, PAIR), BF)
        fill = jnp.zeros((KEY_PAD - key_rows, PAIR), BF)
        for col in range(0, chan_n, PAIR):
            cols = slice(col, col + PAIR)
            keys, vals = kc_ref[:, cols], vc_ref[:, cols]
            keys = jnp.concatenate([jnp.where(key_left, keys, zero), fill, jnp.where(key_left, zero, keys), fill], 0)
            vals = jnp.concatenate([jnp.where(key_left, vals, zero), fill, jnp.where(key_left, zero, vals), fill], 0)
            s = mm_t(q_all[:, cols], keys)
            exps, sums = [], []
            for h in range(2):
                sh = jnp.where(valid, s[:, h * KEY_PAD:(h + 1) * KEY_PAD], -jnp.inf)
                e = jnp.exp2((sh - sh.max(-1, keepdims=True)) * EXP_SCALE)
                exps.append(e.astype(BF))
                sums.append(e.sum(-1, keepdims=True))
            got = mm(jnp.concatenate(exps, 1), vals)
            crossed[:, cols] = (got / jnp.where(left, sums[0], sums[1])).astype(BF)
        mid_old[...] = mid[...]

    def arrive(first=False):
        if first:
            copies[0].wait()
        val = u_ref[...].astype(F32) + (mm(o_ref[...], ow_buf[...]) + ob_ref[layer, 0:1, :])
        mid[...] = val.astype(BF)
        norm_rows(mid, nrm, *affine(ln_ref, (layer, 1)))

    @pl.when(step == 0)
    def _():
        for cp in copies:
            cp.start()
        arrive(True)

    @pl.when(step == 1)
    def _():
        cross(True)
        arrive()

    @pl.when(step == 2)
    def _():
        leave(True)
        cross()
        arrive()

    @pl.when((step > 2) & (step < lat_n))
    def _():
        leave()
        cross()
        arrive()

    @pl.when(step == lat_n)
    def _():
        leave()
        cross()

    @pl.when(step == lat_n + 1)
    def _():
        leave()


def mix_call(o, u, kv, key_n, out_w, out_b, q_t, ln_par, layer):
    lat_n, rows_n, chan_n = u.shape
    blk = (rows_n, chan_n)

    def kv_spec(j):
        return pl.BlockSpec((None, None, None, kv.shape[3], chan_n), lambda i: (layer, j, jnp.clip(i - 1, 0, lat_n - 1), 0, 0))

    return pl.pallas_call(
        functools.partial(mix_kernel, lat_n=lat_n, layer=layer, key_n=key_n),
        grid=(lat_n + 2,),
        in_specs=[lat_spec(blk, lat_n, 0), lat_spec(blk, lat_n, 0), kv_spec(0), kv_spec(1), HBM_SPEC, whole(out_b.shape), HBM_SPEC, whole(ln_par.shape)],
        out_specs=[lat_spec(blk, lat_n, 2), lat_spec(blk, lat_n, 2)],
        out_shape=[jax.ShapeDtypeStruct((lat_n,) + blk, BF)] * 2,
        scratch_shapes=[pltpu.VMEM((chan_n, chan_n), BF)] * 3 + [pltpu.VMEM(blk, BF)] * 4 + [pltpu.SemaphoreType.DMA((3,))],
        compiler_params=params(),
        cost_estimate=pl.CostEstimate(flops=6 * lat_n * rows_n * chan_n * chan_n, bytes_accessed=6 * chan_n * chan_n, transcendentals=0),
        name='mix',
    )(o, u, kv, kv, out_w, out_b, q_t, ln_par)


def gelu(val):
    return 0.5 * val * (1.0 + lax.erf(val * math.sqrt(0.5)))


def ff_kernel(n_hbm, r_hbm, wa_ref, wb_ref, ba_ref, bb_ref, wo_ref, bo_ref, o_hbm, n_buf, r_buf, pa, pb, gate, acc, in_sems, r_sem, out_sems, *, steps, chunk, layer):
    step = pl.program_id(0)
    tok_n = n_buf.shape[0]
    pieces = [pl.ds(i * chunk, chunk) for i in range(tok_n // chunk)]
    loads = [pltpu.make_async_copy(n_hbm.at[p], n_buf.at[p], in_sems.at[i]) for i, p in enumerate(pieces)]
    r_load = pltpu.make_async_copy(r_hbm, r_buf, r_sem)
    stores = [pltpu.make_async_copy(r_buf.at[p], o_hbm.at[p], out_sems.at[i]) for i, p in enumerate(pieces)]

    def widen(first=False):
        for i, p in enumerate(pieces):
            if first:
                loads[i].wait()
            pa[p, :] = mm(n_buf[p, :], wa_ref[...])
            pb[p, :] = mm(n_buf[p, :], wb_ref[...])

    def activate():
        for p in pieces:
            gate[p, :] = ((pa[p, :] + ba_ref[layer:layer + 1, :]) * gelu(pb[p, :] + bb_ref[layer:layer + 1, :])).astype(BF)

    def narrow(first=False):
        for p in pieces:
            val = mm(gate[p, :], wo_ref[...])
            if first:
                acc[p, :] = val
            else:
                acc[p, :] += val

    @pl.when(step == 0)
    def _():
        for cp in loads:
            cp.start()
        widen(True)

    @pl.when(step == 1)
    def _():
        r_load.start()
        activate()
        widen()

    @pl.when(step == 2)
    def _():
        narrow(True)
        activate()
        widen()

    @pl.when((step > 2) & (step < steps))
    def _():
        narrow()
        activate()
        widen()

    @pl.when(step == steps)
    def _():
        narrow()
        activate()

    @pl.when(step == steps + 1)
    def _():
        r_load.wait()
        for i, p in enumerate(pieces):
            val = acc[p, :] + mm(gate[p, :], wo_ref[...]) + bo_ref[layer:layer + 1, :]
            r_buf[p, :] = (r_buf[p, :].astype(F32) + val).astype(BF)
            stores[i].start()
        for cp in stores:
            cp.wait()


def ff_call(nrm, res, w_in, b_in, w_out, b_out, layer, fb=512, chunk=512):
    tok_n, chan_n = nrm.shape
    ff_n = w_out.shape[1]
    steps = ff_n // fb
    now = lambda s: jnp.minimum(s, steps - 1)
    act = lambda s: jnp.clip(s - 1, 0, steps - 1)
    return pl.pallas_call(
        functools.partial(ff_kernel, steps=steps, chunk=chunk, layer=layer),
        grid=(steps + 2,),
        in_specs=[HBM_SPEC, HBM_SPEC,
                  pl.BlockSpec((None, chan_n, fb), lambda s: (layer, 0, now(s))),
                  pl.BlockSpec((None, chan_n, fb), lambda s: (layer, 0, steps + now(s))),
                  pl.BlockSpec((b_in.shape[0], fb), lambda s: (0, act(s))),
                  pl.BlockSpec((b_in.shape[0], fb), lambda s: (0, steps + act(s))),
                  pl.BlockSpec((None, fb, chan_n), lambda s: (layer, jnp.maximum(s - 2, 0), 0)),
                  whole(b_out.shape)],
        out_specs=HBM_SPEC,
        out_shape=jax.ShapeDtypeStruct((tok_n, chan_n), BF),
        scratch_shapes=[pltpu.VMEM((tok_n, chan_n), BF)] * 2 + [pltpu.VMEM((tok_n, fb), F32)] * 2 + [pltpu.VMEM((tok_n, fb), BF), pltpu.VMEM((tok_n, chan_n), F32), pltpu.SemaphoreType.DMA((tok_n // chunk,)), pltpu.SemaphoreType.DMA, pltpu.SemaphoreType.DMA((tok_n // chunk,))],
        compiler_params=params(),
        cost_estimate=pl.CostEstimate(flops=6 * tok_n * chan_n * ff_n, bytes_accessed=6 * chan_n * ff_n, transcendentals=0),
        name='ff',
    )(nrm, res, w_in, w_in, b_in, b_in, w_out, b_out)


def exit_kernel(u_ref, h_ref, pw_hbm, pb_ref, norm_ref, tog_ref, toc_ref, m_ref, x_ref, pw_buf, held, sems, *, lat_n, eps_val, at):
    step = pl.program_id(0)
    chan_n = held.shape[1]
    half = chan_n // 2
    copies = [pltpu.make_async_copy(pw_hbm.at[1, pl.ds(i * half, half)], pw_buf.at[pl.ds(i * half, half)], sems.at[i]) for i in range(2)]

    def project(first=False):
        if first:
            copies[0].wait()
            val = mm(u_ref[:, 0:half], pw_buf[0:half])
            copies[1].wait()
            val = val + mm(u_ref[:, half:], pw_buf[half:])
        else:
            val = mm(u_ref[...], pw_buf[...])
        val = (val + pb_ref[1:2, :] + h_ref[...].astype(F32)).astype(BF)
        held[...] = val
        m_ref[...] = val

    def finish():
        norm_latent(held, x_ref, *affine(norm_ref, at), tog_ref[...], toc_ref[...], eps_val, True)

    @pl.when(step == 0)
    def _():
        for cp in copies:
            cp.start()
        project(True)

    @pl.when((step > 0) & (step < lat_n))
    def _():
        finish()
        project()

    @pl.when(step == lat_n)
    def _():
        finish()


def exit_call(u, h, proj_w, proj_b, norm, at, eps_val):
    lat_n, rows_n, chan_n = u.shape
    to_group, to_chan = group_tables(chan_n)
    blk = (rows_n, chan_n)
    return pl.pallas_call(
        functools.partial(exit_kernel, lat_n=lat_n, eps_val=eps_val, at=at),
        grid=(lat_n + 1,),
        in_specs=[lat_spec(blk, lat_n, 0), lat_spec(blk, lat_n, 0), HBM_SPEC, whole(proj_b.shape), whole(norm.shape), whole((chan_n, 128)), whole((128, chan_n))],
        out_specs=[lat_spec(blk, lat_n, 0), lat_spec((rows_n, 3 * chan_n), lat_n, 1)],
        out_shape=[jax.ShapeDtypeStruct((lat_n,) + blk, BF), jax.ShapeDtypeStruct((lat_n, rows_n, 3 * chan_n), BF)],
        scratch_shapes=[pltpu.VMEM((chan_n, chan_n), BF), pltpu.VMEM(blk, BF), pltpu.SemaphoreType.DMA((2,))],
        compiler_params=params(),
        cost_estimate=pl.CostEstimate(flops=2 * lat_n * rows_n * chan_n * chan_n, bytes_accessed=2 * chan_n * chan_n, transcendentals=0),
        name='exit',
    )(u, h, proj_w, proj_b, norm, to_group, to_chan)


def device_block(latents, time_emb, context, res_norm, res_conv_w, res_conv_b, res_temb_w, res_temb_b, tr_norm, proj_w, proj_b, ln_par, self_qkv, cross_q, cross_kv, attn_out, attn_b, ff_in_w, ff_in_b, ff_out_w, ff_out_b, sp_size):
    lat_all, band_n, width_n, chan_n = latents.shape
    own_n = lat_all // sp_size
    tok_n = band_n * sp_size * width_n
    first = lax.axis_index('sp') * own_n
    whole_lat = lax.all_to_all(latents, 'sp', 0, 1, tiled=True).reshape(own_n, tok_n, chan_n)
    time_own = lax.dynamic_slice_in_dim(time_emb, first, own_n, 0)
    ctx_own = lax.dynamic_slice_in_dim(context, first, own_n, 0)
    key_n = ctx_own.shape[1]
    ctx_pad = jnp.pad(ctx_own, ((0, 0), (0, -key_n % 16), (0, 0)))

    conv_w = res_conv_w.reshape(4, 9 * chan_n, chan_n)
    qkv_t = self_qkv.transpose(0, 1, 3, 4, 2).reshape(2, 3, chan_n, chan_n)
    cross_q_t = cross_q.transpose(0, 2, 3, 1).reshape(2, chan_n, chan_n)
    cross_kv_t = cross_kv.transpose(0, 1, 3, 4, 2).reshape(2, 2, chan_n, -1)
    out_w = attn_out.reshape(2, 2, chan_n, chan_n)
    trunk_norm = tr_norm[None]

    kv = jnp.einsum('btc,ljdc->ljbtd', ctx_pad, cross_kv_t, preferred_element_type=F32).astype(BF)
    time_act = jax.nn.silu(time_own.astype(F32)).astype(BF)
    time_rows = [(jnp.dot(time_act, res_temb_w[r], preferred_element_type=F32) + res_temb_b[r])[:, None, :] for r in range(2)]

    spread = prep_call(whole_lat, res_norm, (0, 0), 1e-5)
    spread, = conv_call(spread, conv_w, 0, res_conv_b, time_rows[0], None, res_norm, (0, 1), 1e-5, True)
    hidden, normed = conv_call(spread, conv_w, 1, res_conv_b, None, whole_lat, trunk_norm, (0,), 1e-6, False)
    for layer in range(2):
        if layer == 0:
            tokens, qkv = enter_call(normed, proj_w, proj_b, ln_par, qkv_t, 0)
        else:
            qkv = heads_call(tokens, ln_par, qkv_t, layer)
        attended = attn_call(qkv)
        tokens, normed = mix_call(attended, tokens, kv, key_n, out_w, attn_b, cross_q_t, ln_par, layer)
        flat = (own_n * tok_n, chan_n)
        tokens = ff_call(normed.reshape(flat), tokens.reshape(flat), ff_in_w, ff_in_b, ff_out_w, ff_out_b, layer).reshape(own_n, tok_n, chan_n)
    middle, spread = exit_call(tokens, hidden, proj_w, proj_b, res_norm, (1, 0), 1e-5)
    spread, = conv_call(spread, conv_w, 2, res_conv_b, time_rows[1], None, res_norm, (1, 1), 1e-5, True)
    last, = conv_call(spread, conv_w, 3, res_conv_b, None, middle, None, None, 0.0, False)
    return lax.all_to_all(last.reshape(own_n, band_n * sp_size, width_n, chan_n), 'sp', 1, 0, tiled=True)


def solution(mesh):
    sp_size = mesh.shape['sp']
    row_spec = P('dp', 'sp')
    part_spec = P('dp')
    in_specs = (row_spec, part_spec, part_spec) + (P(),) * 18
    body_fn = functools.partial(device_block, sp_size=sp_size)
    return jax.shard_map(body_fn, mesh=mesh, in_specs=in_specs, out_specs=row_spec, check_vma=False)
```
